64 devices in a mesh: rep: 4 (over x, y), dp: 16 (over z, core).
Axes of the slice: x: 2, y: 2, z: 8, core: 2. Of those that a mesh axis runs over, the one named last changes fastest.
The devices are a block of a 4x4x8 slice.
Arguments:
- x: bfloat16 [64, 2048, 512], P(('rep', 'dp')), parts along dimension 0
- dy: bfloat16 [64, 2048, 512], P(('rep', 'dp')), parts along dimension 0
- wq: bfloat16 [2, 512, 768], P(None, 'dp')
- wk: bfloat16 [2, 512, 128], P(None, 'dp')
- wv: bfloat16 [2, 512, 128], P(None, 'dp')
- wo: bfloat16 [2, 768, 512], P(None, 'dp')
- w_gate: bfloat16 [2, 512, 2048], P(None, 'dp')
- w_up: bfloat16 [2, 512, 2048], P(None, 'dp')
- w_down: bfloat16 [2, 2048, 512], P(None, 'dp')
- m_wq: float32 [2, 512, 768], P(None, 'dp')
- m_wk: float32 [2, 512, 128], P(None, 'dp')
- m_wv: float32 [2, 512, 128], P(None, 'dp')
- m_wo: float32 [2, 768, 512], P(None, 'dp')
- m_w_gate: float32 [2, 512, 2048], P(None, 'dp')
- m_w_up: float32 [2, 512, 2048], P(None, 'dp')
- m_w_down: float32 [2, 2048, 512], P(None, 'dp')
- v_wq: float32 [2, 512, 768], P(None, 'dp')
- v_wk: float32 [2, 512, 128], P(None, 'dp')
- v_wv: float32 [2, 512, 128], P(None, 'dp')
- v_wo: float32 [2, 768, 512], P(None, 'dp')
- v_w_gate: float32 [2, 512, 2048], P(None, 'dp')
- v_w_up: float32 [2, 512, 2048], P(None, 'dp')
- v_w_down: float32 [2, 2048, 512], P(None, 'dp')
Outputs:
- output 1: bfloat16 [8, 512, 768], P('rep', 'dp'), parts along dimension 0
- output 2: bfloat16 [8, 512, 128], P('rep', 'dp'), parts along dimension 0
- output 3: bfloat16 [8, 512, 128], P('rep', 'dp'), parts along dimension 0
- output 4: bfloat16 [8, 768, 512], P('rep', 'dp'), parts along dimension 0
- output 5: bfloat16 [8, 512, 2048], P('rep', 'dp'), parts along dimension 0
- output 6: bfloat16 [8, 512, 2048], P('rep', 'dp'), parts along dimension 0
- output 7: bfloat16 [8, 2048, 512], P('rep', 'dp'), parts along dimension 0
- output 8: float32 [8, 512, 768], P('rep', 'dp'), parts along dimension 0
- output 9: float32 [8, 512, 128], P('rep', 'dp'), parts along dimension 0
- output 10: float32 [8, 512, 128], P('rep', 'dp'), parts along dimension 0
- output 11: float32 [8, 768, 512], P('rep', 'dp'), parts along dimension 0
- output 12: float32 [8, 512, 2048], P('rep', 'dp'), parts along dimension 0
- output 13: float32 [8, 512, 2048], P('rep', 'dp'), parts along dimension 0
- output 14: float32 [8, 2048, 512], P('rep', 'dp'), parts along dimension 0
- output 15: float32 [8, 512, 768], P('rep', 'dp'), parts along dimension 0
- output 16: float32 [8, 512, 128], P('rep', 'dp'), parts along dimension 0
- output 17: float32 [8, 512, 128], P('rep', 'dp'), parts along dimension 0
- output 18: float32 [8, 768, 512], P('rep', 'dp'), parts along dimension 0
- output 19: float32 [8, 512, 2048], P('rep', 'dp'), parts along dimension 0
- output 20: float32 [8, 512, 2048], P('rep', 'dp'), parts along dimension 0
- output 21: float32 [8, 2048, 512], P('rep', 'dp'), parts along dimension 0
There are 4 independent parts. The reference program is written for one: setup_inputs(seed, part) draws one part's arguments, and reference() takes and returns one part's arrays. A program takes and returns all parts, laid end to end along the dimension named above; an argument that names none is the same for every part.
All inputs are finite; a program needn't handle non-finite values.
Results may differ from the reference program's by a relative error of at most 0.0245.
Values are sent between devices in bfloat16 or wider.
A program may use at most 768 MiB of HBM per device.

```python
import jax
import jax.numpy as jnp
from jax import lax

SEQUENCES = 16
TOKENS = 2048
D = 512
HEADS = 6
KV_HEADS = 1
HEAD = 128
FF = 2048
LAYERS = 2
THETA = 10000
NAMES = ("wq", "wk", "wv", "wo", "w_gate", "w_up", "w_down")
SHAPES = {
    "wq": (LAYERS, D, HEADS * HEAD),
    "wk": (LAYERS, D, KV_HEADS * HEAD),
    "wv": (LAYERS, D, KV_HEADS * HEAD),
    "wo": (LAYERS, HEADS * HEAD, D),
    "w_gate": (LAYERS, D, FF),
    "w_up": (LAYERS, D, FF),
    "w_down": (LAYERS, FF, D),
}


def bump(key, n, height):
    away = (jnp.arange(n, dtype=jnp.int32) - jax.random.randint(key, (), 0, n, jnp.int32)) % n
    return jnp.where(away < n // 8, height, 1.0)


def together(key, own, strength):
    shared = jax.random.normal(key, own.shape[1:], jnp.float32)
    return (own + strength * shared) * lax.rsqrt(1 + strength * strength)


def setup_inputs(seed: int = 0, part: int = 0) -> dict:
    kx, kdy, ka, kb, kz, kf, kh, kl, *keys = jax.random.split(jax.random.key(seed), 8 + 3 * len(NAMES))
    kx, kdy, ka, kb = (jax.random.fold_in(k, part) for k in (kx, kdy, ka, kb))
    kw, km, kv = (keys[i::3] for i in range(3))
    shape = (SEQUENCES, TOKENS, D)
    much_x, much_dy = jax.random.uniform(kz, (2,), jnp.float32, 0.0, 1.0)
    loud = 2.0 ** jax.random.uniform(jax.random.fold_in(kz, 1), (), jnp.float32, -1.0, 2.0)
    layers = 2.0 ** jax.random.uniform(kl, (LAYERS, 1, 1), jnp.float32, -1.0, 1.0)
    times = {"wq": 1.0, "wk": 1.0, "wv": 2.0, "wo": layers, "w_gate": 1.0, "w_up": bump(kh, FF, 4.0), "w_down": layers}
    x = together(ka, jax.random.normal(kx, shape, jnp.float32), much_x) * bump(kf, D, 4.0)
    dy = together(kb, jax.random.normal(kdy, shape, jnp.float32), much_dy)
    drawn = {"x": x.astype(jnp.bfloat16), "dy": (loud * dy * (SEQUENCES * TOKENS) ** -0.5).astype(jnp.bfloat16)}
    for key, name in zip(kw, NAMES, strict=True):
        drawn[name] = (jax.random.normal(key, SHAPES[name], jnp.float32) * SHAPES[name][1] ** -0.5 * times[name]).astype(jnp.bfloat16)
    for key, name in zip(km, NAMES, strict=True):
        drawn[f"m_{name}"] = 0.1 * jax.random.normal(key, SHAPES[name], jnp.float32)
    for key, name in zip(kv, NAMES, strict=True):
        drawn[f"v_{name}"] = jax.random.uniform(key, SHAPES[name], jnp.float32, 0.02, 0.06)
    return drawn


def matmul(a, w):
    return jnp.dot(a, w, preferred_element_type=jnp.float32).astype(jnp.bfloat16)


def normed(h):
    wide = h.astype(jnp.float32)
    scale = lax.rsqrt(jnp.mean(wide**2, -1, keepdims=True) + 1e-6)
    return (wide * scale).astype(jnp.bfloat16)


def turned(t, theta):
    half = t.shape[-1] // 2
    angle = jnp.arange(t.shape[0], dtype=jnp.float32)[:, None] * theta ** (-jnp.arange(half, dtype=jnp.float32) / half)
    cos, sin = jnp.cos(angle)[:, None], jnp.sin(angle)[:, None]
    a, b = t[..., :half].astype(jnp.float32), t[..., half:].astype(jnp.float32)
    return jnp.concatenate([a * cos - b * sin, b * cos + a * sin], -1).astype(jnp.bfloat16)


def seen_by(q, k, v):
    tokens, kv = q.shape[0], k.shape[1]
    q = q.reshape(tokens, kv, -1, q.shape[-1])
    scores = jnp.einsum("tgsd,ugd->gstu", q.astype(jnp.float32), k.astype(jnp.float32)) * q.shape[-1] ** -0.5
    place = jnp.arange(tokens)
    weights = jax.nn.softmax(jnp.where(place[:, None] >= place, scores, -jnp.inf), -1).astype(jnp.bfloat16)
    return jnp.einsum("gstu,ugd->tgsd", weights.astype(jnp.float32), v.astype(jnp.float32)).astype(jnp.bfloat16).reshape(tokens, -1)


def layer(h, w):
    a = normed(h)
    q, k = (turned(matmul(a, w[name]).reshape(h.shape[0], -1, HEAD), THETA) for name in ("wq", "wk"))
    h = h + matmul(seen_by(q, k, matmul(a, w["wv"]).reshape(h.shape[0], -1, HEAD)), w["wo"])
    b = normed(h)
    gate = jnp.dot(b, w["w_gate"], preferred_element_type=jnp.float32)
    up = jnp.dot(b, w["w_up"], preferred_element_type=jnp.float32)
    return h + matmul((jax.nn.silu(gate) * up).astype(jnp.bfloat16), w["w_down"])


def adamw(w, m, v, g):
    m = 0.9 * m + 0.1 * g
    v = 0.95 * v + 0.05 * g * g
    step = m * lax.rsqrt(v + 1e-8) + 0.1 * w
    return (w - 0.02 * step).astype(jnp.bfloat16), m, v


def clipped(gradients, sum_of_squares, count):
    factor = jnp.minimum(1.0, 0.5 * lax.rsqrt(sum_of_squares / count + 1e-30))
    return [g * factor for g in gradients]


def stack(weights, h):
    return lax.scan(lambda h, w: (layer(h, w), None), h, weights)[0]


def reference(x, dy, wq, wk, wv, wo, w_gate, w_up, w_down, m_wq, m_wk, m_wv, m_wo, m_w_gate, m_w_up, m_w_down, v_wq, v_wk, v_wv, v_wo, v_w_gate, v_w_up, v_w_down):
    weights = dict(zip(NAMES, (wq, wk, wv, wo, w_gate, w_up, w_down), strict=True))

    def take(so_far, sequence):
        h, by_y = sequence
        _, back = jax.vjp(stack, weights, h)
        by_weights, by_h = back(by_y)
        return jax.tree.map(lambda total, term: total + term.astype(jnp.float32), so_far, by_weights), by_h

    none_yet = {name: jnp.zeros(w.shape, jnp.float32) for name, w in weights.items()}
    by_weights, by_x = lax.scan(take, none_yet, (x, dy))
    gradients = [by_weights[name].astype(jnp.bfloat16).astype(jnp.float32) for name in NAMES]
    gradients = clipped(gradients, sum(jnp.sum(g * g) for g in gradients), sum(g.size for g in gradients))
    first = (m_wq, m_wk, m_wv, m_wo, m_w_gate, m_w_up, m_w_down)
    second = (v_wq, v_wk, v_wv, v_wo, v_w_gate, v_w_up, v_w_down)
    new = [adamw(weights[name].astype(jnp.float32), m, v, g) for name, m, v, g in zip(NAMES, first, second, gradients, strict=True)]
    return tuple(one[which] for which in range(3) for one in new)
```

```python
import functools

import jax
import jax.numpy as jnp
from jax import lax
from jax.experimental import pallas as pl
from jax.experimental.pallas import tpu as pltpu
from jax.sharding import PartitionSpec as P

NEG = -1e30
LOG2E = 1.4426950408889634
VMEM = 58 * 2**20
HEAD = 128
THETA = 10000
BLOCK = 512
BF, F32 = jnp.bfloat16, jnp.float32


def _dot(a, b, ca=1, cb=0):
    return lax.dot_general(a, b, (((ca,), (cb,)), ((), ())), preferred_element_type=F32)


def _scale(x):
    return lax.rsqrt(jnp.mean(x * x, -1, keepdims=True) + 1e-6)


def _norm_back(x, r, d):
    y = x * r
    return r * (d - y * jnp.mean(d * y, -1, keepdims=True))


def _turn(t, cos, sin, back=False):
    t = t.astype(F32)
    other = pltpu.roll(t, HEAD // 2, 1) * sin
    return (t * cos - other if back else t * cos + other).astype(BF)


def _unpack_wo(w_ref, wo_s, at, n):
    d = w_ref.shape[0]
    r, each, half = d // n, wo_s.shape[0] // n, d // 2
    rest = each - r
    for i in range(n):
        wo_s[i * each : i * each + r, :] = w_ref[i * r : (i + 1) * r, at : at + d]
        wo_s[i * each + r : (i + 1) * each, :half] = w_ref[i * r : i * r + rest, at + d : at + d + half]
        wo_s[i * each + r : (i + 1) * each, half:] = w_ref[i * r + rest : (i + 1) * r, at + d : at + d + half]


def _unpack_wd(w_ref, wd_s, at, n):
    d = w_ref.shape[0]
    r, each = d // n, wd_s.shape[0] // n
    for i in range(n):
        for q in range(each // r):
            wd_s[i * each + q * r : i * each + (q + 1) * r, :] = w_ref[i * r : (i + 1) * r, at + q * d : at + (q + 1) * d]


def _gap(b):
    return lax.broadcasted_iota(jnp.int32, (b, b), 1) - lax.broadcasted_iota(jnp.int32, (b, b), 0)


def _attn_forward(h_ref, w_ref, cos_ref, sin_ref, q_ref, k_ref, v_ref, o_ref, lse_ref, mid_ref, k_s, vt_s, top_s, mix_s, gap_s, wo_s, *, n, heads):
    i = pl.program_id(0)
    b, hd = h_ref.shape[0], heads * HEAD
    e = HEAD**-0.5 * LOG2E

    @pl.when(i == 0)
    def _():
        gap_s[...] = _gap(b)
        vt_s[HEAD:, :] = jnp.ones((vt_s.shape[0] - HEAD, vt_s.shape[1]), BF)
        _unpack_wo(w_ref, wo_s, hd + 2 * HEAD, n)

    here = pl.ds(pl.multiple_of(i * b, b), b)
    x = h_ref[...].astype(F32)
    a = (x * _scale(x)).astype(BF)
    cos, sin = cos_ref[...], sin_ref[...]
    kv = _dot(a, w_ref[:, hd : hd + 2 * HEAD]).astype(BF)
    k = _turn(kv[:, :HEAD], cos, sin)
    v = kv[:, HEAD:]
    k_ref[...] = k
    v_ref[...] = v
    k_s[here, :] = k
    vt_s[:HEAD, here] = v.T
    for m in range(heads):
        at = slice(m * HEAD, (m + 1) * HEAD)
        q_ref[:, at] = _turn(_dot(a, w_ref[:, at]).astype(BF), cos, sin)
    top_s[...] = jnp.full(top_s.shape, NEG, F32)
    mix_s[...] = jnp.zeros(mix_s.shape, F32)

    def block(start, keys, cut, masked):
        there = pl.ds(pl.multiple_of(start, keys), keys)
        kj, vj = k_s[there, :], vt_s[:, there]
        scores = [_dot(kj, q_ref[cut:, m * HEAD : (m + 1) * HEAD], 1, 1) for m in range(heads)]
        ps, keeps = [], []
        for m, s in enumerate(scores):
            if masked:
                s = jnp.where(gap_s[:keys, : b - cut] >= 0, s, 2 * NEG)
            old = top_s[m : m + 1, cut:]
            top = jnp.maximum(old, s.max(axis=0, keepdims=True))
            top_s[m : m + 1, cut:] = top
            ps.append(jnp.exp2((s - top) * e).astype(BF))
            keeps.append(jnp.exp2((old - top) * e))
        for m in range(heads):
            mix_s[m, :, cut:] = mix_s[m, :, cut:] * keeps[m] + _dot(vj, ps[m])

    lax.fori_loop(0, i, lambda j, _: block(j * b, b, 0, False), None)
    block(i * b, b // 2, 0, True)
    block(i * b + b // 2, b // 2, b // 2, True)
    for m in range(heads):
        total = mix_s[m, HEAD : HEAD + 1, :]
        o_ref[:, m * HEAD : (m + 1) * HEAD] = (mix_s[m, :HEAD, :] * (1 / total)).T.astype(BF)
        lse_ref[m : m + 1, :] = top_s[m : m + 1, :] * e + jnp.log(total) * LOG2E
    lse_ref[heads:, :] = jnp.zeros((lse_ref.shape[0] - heads, b), F32)
    mid_ref[...] = (x + _dot(o_ref[...], wo_s[...]).astype(BF).astype(F32)).astype(BF)


def _attn_backward(*refs, n, heads, need):
    dm_ref, h_ref, q_ref, k_ref, v_ref, o_ref, lse_ref, w_ref, cos_ref, sin_ref = refs[:10]
    refs = refs[10:]
    dh_ref, refs = (refs[0], refs[1:]) if need else (None, refs)
    g_ref, dk_s, dv_s, dq_s, do_s, wqkv_s, dwo_s, wo_s, kt_s, gap_s = refs
    step, blocks = pl.program_id(0), pl.num_programs(0)
    i = blocks - 1 - step
    b, d = dm_ref.shape
    hd = heads * HEAD
    wide = hd + 2 * HEAD
    scale = HEAD**-0.5
    e = scale * LOG2E

    @pl.when(step == 0)
    def _():
        gap_s[...] = _gap(b)
        dk_s[...] = jnp.zeros(dk_s.shape, F32)
        dv_s[...] = jnp.zeros(dv_s.shape, F32)
        wqkv_s[...] = jnp.zeros(wqkv_s.shape, F32)
        dwo_s[...] = jnp.zeros(dwo_s.shape, F32)
        kt_s[...] = k_ref[...].T
        _unpack_wo(w_ref, wo_s, wide, n)

    dm = dm_ref[...]
    do_s[...] = _dot(dm, wo_s[...], 1, 1).astype(BF)
    dwo_s[...] += _dot(o_ref[...], dm, 0, 0)
    dq_s[...] = jnp.zeros(dq_s.shape, F32)
    deltas = []
    for m in range(heads):
        at = slice(m * HEAD, (m + 1) * HEAD)
        deltas.append((do_s[:, at].astype(F32) * o_ref[:, at].astype(F32)).T.sum(axis=0, keepdims=True))

    def block(start, keys, cut, masked):
        there = pl.ds(pl.multiple_of(start, keys), keys)
        kj, vj, ktj = k_ref[there, :], v_ref[there, :], kt_s[:, there]
        lanes = [slice(m * HEAD, (m + 1) * HEAD) for m in range(heads)]
        scores = [_dot(kj, q_ref[cut:, at], 1, 1) for at in lanes]
        dps = [_dot(vj, do_s[cut:, at], 1, 1) for at in lanes]
        for m, at in enumerate(lanes):
            p = jnp.exp2(scores[m] * e - lse_ref[m : m + 1, cut:])
            if masked:
                p = jnp.where(gap_s[:keys, : b - cut] >= 0, p, 0.0)
            ds = (p * (dps[m] - deltas[m][:, cut:])).astype(BF)
            dv_s[there, :] += _dot(p.astype(BF), do_s[cut:, at])
            dk_s[there, :] += _dot(ds, q_ref[cut:, at])
            dq_s[m, :, cut:] += _dot(ktj, ds)

    lax.fori_loop(0, i, lambda j, _: block(j * b, b, 0, False), None)
    block(i * b, b // 2, 0, True)
    block(i * b + b // 2, b // 2, b // 2, True)

    here = pl.ds(pl.multiple_of(i * b, b), b)
    cos, sin = cos_ref[...], sin_ref[...]
    parts = [_turn((dq_s[m] * scale).T.astype(BF), cos, sin, True) for m in range(heads)]
    parts += [_turn((dk_s[here, :] * scale).astype(BF), cos, sin, True), dv_s[here, :].astype(BF)]
    dqkv = jnp.concatenate(parts, axis=1)
    x = h_ref[...].astype(F32)
    r = _scale(x)
    wqkv_s[...] += _dot((x * r).astype(BF), dqkv, 0, 0)
    if need:
        da = _dot(dqkv, w_ref[:, :wide], 1, 1).astype(BF).astype(F32)
        dh_ref[...] = (dm.astype(F32) + _norm_back(x, r, da)).astype(BF)

    @pl.when(step == blocks - 1)
    def _():
        rows, each, half = d // n, hd // n, d // 2
        rest = each - rows
        g_ref[:, :wide] = wqkv_s[...].astype(BF)
        for m in range(n):
            g_ref[m * rows : (m + 1) * rows, wide : wide + d] = dwo_s[m * each : m * each + rows, :].astype(BF)
            tail = dwo_s[m * each + rows : (m + 1) * each, :].astype(BF)
            g_ref[m * rows : m * rows + rest, wide + d : wide + d + half] = tail[:, :half]
            g_ref[m * rows + rest : (m + 1) * rows, wide + d : wide + d + half] = tail[:, half:]


def _mlp_forward(h_ref, w_ref, y_ref, wd_s, *, n, ff, base):
    d = h_ref.shape[1]

    @pl.when(pl.program_id(0) == 0)
    def _():
        _unpack_wd(w_ref, wd_s, base + 2 * ff, n)

    x = h_ref[...].astype(F32)
    a = (x * _scale(x)).astype(BF)
    y = None
    for c in range(0, ff, d):
        gate, up = (_dot(a, w_ref[:, at : at + d]) for at in (base + c, base + ff + c))
        part = _dot((gate * jax.nn.sigmoid(gate) * up).astype(BF), wd_s[c : c + d, :])
        y = part if y is None else y + part
    y_ref[...] = (x + y.astype(BF).astype(F32)).astype(BF)


def _mlp_backward(dy_ref, h_ref, w_ref, *refs, n, ff, base, join):
    g_in, refs = (refs[0], refs[1:]) if join else (None, refs)
    dh_ref, g_ref, wd_s, dgu_s, dwd_s = refs
    d = h_ref.shape[1]
    step, blocks = pl.program_id(0), pl.num_programs(0)

    @pl.when(step == 0)
    def _():
        _unpack_wd(w_ref, wd_s, base + 2 * ff, n)
        dgu_s[...] = jnp.zeros(dgu_s.shape, F32)
        dwd_s[...] = jnp.zeros(dwd_s.shape, F32)

    x = h_ref[...].astype(F32)
    r = _scale(x)
    a = (x * r).astype(BF)
    dy = dy_ref[...]
    at, dyt = a.T, dy.T
    da = None
    for c in range(0, ff, d):
        wg, wu = (w_ref[:, m : m + d] for m in (base + c, base + ff + c))
        gate, up = _dot(a, wg), _dot(a, wu)
        du = _dot(dy, wd_s[c : c + d, :], 1, 1).astype(BF).astype(F32)
        s = jax.nn.sigmoid(gate)
        silu = gate * s
        u = (silu * up).astype(BF)
        dup = (du * silu).astype(BF)
        dgate = (du * up * (s * (1 + gate * (1 - s)))).astype(BF)
        part = _dot(dgate, wg, 1, 1) + _dot(dup, wu, 1, 1)
        da = part if da is None else da + part
        dgu_s[:, c : c + d] += _dot(at, dgate)
        dgu_s[:, ff + c : ff + c + d] += _dot(at, dup)
        dwd_s[:, c : c + d] += _dot(dyt, u)
    da = da.astype(BF).astype(F32)
    dh_ref[...] = (dy.astype(F32) + _norm_back(x, r, da)).astype(BF)

    @pl.when(step == blocks - 1)
    def _():
        rows, each = d // n, ff // n
        g_ref[:, : 2 * ff] = dgu_s[...].astype(BF)
        if join:
            g_ref[:, 2 * ff + (each // rows) * d :] = g_in[...]
        for m in range(n):
            own = dwd_s[:, m * each : (m + 1) * each].T.astype(BF)
            for q in range(each // rows):
                at_q = 2 * ff + q * d
                g_ref[m * rows : (m + 1) * rows, at_q : at_q + d] = own[q * rows : (q + 1) * rows, :]


def _whole(shape):
    return pl.BlockSpec(shape, lambda i: (0,) * len(shape), pipeline_mode=pl.Buffered(1))


def _params():
    return pltpu.CompilerParams(dimension_semantics=("arbitrary",), vmem_limit_bytes=VMEM)


def _cost(flops, exps, arrays):
    return pl.CostEstimate(flops=flops, transcendentals=exps, bytes_accessed=sum(a.size * a.dtype.itemsize for a in arrays))


def attn_forward(h, w, cos, sin, n, heads):
    t, d = h.shape
    b, hd = BLOCK, heads * HEAD
    rows = lambda width: pl.BlockSpec((b, width), lambda i: (i, 0))
    shape = jax.ShapeDtypeStruct
    return pl.pallas_call(
        functools.partial(_attn_forward, n=n, heads=heads),
        grid=(t // b,),
        in_specs=[rows(d), _whole((d, hd + 2 * HEAD + d + d // 2)), rows(HEAD), rows(HEAD)],
        out_specs=[rows(hd), rows(HEAD), rows(HEAD), rows(hd), pl.BlockSpec((8, b), lambda i: (0, i)), rows(d)],
        out_shape=[shape((t, hd), BF), shape((t, HEAD), BF), shape((t, HEAD), BF), shape((t, hd), BF), shape((8, t), F32), shape((t, d), BF)],
        scratch_shapes=[pltpu.VMEM((t, HEAD), BF), pltpu.VMEM((HEAD + 16, t), BF), pltpu.VMEM((8, b), F32), pltpu.VMEM((heads, HEAD + 16, b), F32),
                        pltpu.VMEM((b, b), jnp.int32), pltpu.VMEM((hd, d), BF)],
        compiler_params=_params(),
        cost_estimate=_cost(2 * t * w.size + 4 * heads * t * t * HEAD, heads * t * t, [h, w, h, h, h]),
        name="attn_forward",
    )(h, w, cos, sin)


def attn_backward(dm, h, q, k, v, o, lse, w, cos, sin, n, need):
    t, d = h.shape
    b, hd = BLOCK, q.shape[1]
    heads = hd // HEAD
    wide = hd + 2 * HEAD
    last = t // b - 1
    rows = lambda width: pl.BlockSpec((b, width), lambda i: (last - i, 0))
    given = [dm, h, q, k, v, o, lse, w, cos, sin]
    columns = wide + d + d // 2
    g = jax.ShapeDtypeStruct((d, columns), BF)
    outs = ([(jax.ShapeDtypeStruct((t, d), BF), rows(d))] if need else []) + [(g, _whole(g.shape))]
    got = pl.pallas_call(
        functools.partial(_attn_backward, n=n, heads=heads, need=need),
        grid=(t // b,),
        in_specs=[rows(d), rows(d), rows(hd), _whole(k.shape), _whole(v.shape), rows(hd), pl.BlockSpec((8, b), lambda i: (0, last - i)),
                  _whole((d, columns)), rows(HEAD), rows(HEAD)],
        out_specs=[spec for _, spec in outs],
        out_shape=[shape for shape, _ in outs],
        scratch_shapes=[pltpu.VMEM((t, HEAD), F32), pltpu.VMEM((t, HEAD), F32), pltpu.VMEM((heads, HEAD, b), F32), pltpu.VMEM((b, hd), BF),
                        pltpu.VMEM((d, wide), F32), pltpu.VMEM((hd, d), F32), pltpu.VMEM((hd, d), BF), pltpu.VMEM((HEAD, t), BF),
                        pltpu.VMEM((b, b), jnp.int32)],
        compiler_params=_params(),
        cost_estimate=_cost(4 * t * d * columns + 10 * heads * t * t * HEAD, heads * t * t, given),
        name="attn_backward",
    )(*given)
    return got if need else (None, got[0])


def mlp_forward(h, w, n, ff, base):
    t, d = h.shape
    rows = pl.BlockSpec((BLOCK, d), lambda i: (i, 0))
    return pl.pallas_call(
        functools.partial(_mlp_forward, n=n, ff=ff, base=base),
        grid=(t // BLOCK,),
        in_specs=[rows, _whole(w.shape)],
        out_specs=rows,
        out_shape=jax.ShapeDtypeStruct((t, d), BF),
        scratch_shapes=[pltpu.VMEM((ff, d), BF)],
        compiler_params=_params(),
        cost_estimate=_cost(2 * t * w.size, t * ff, [h, h, w]),
        name="mlp_forward",
    )(h, w)


def mlp_backward(dy, h, w, n, ff, base, join):
    t, d = h.shape
    rows = pl.BlockSpec((BLOCK, d), lambda i: (i, 0))
    more = [] if join is None else [join]
    g = jax.ShapeDtypeStruct((d, 2 * ff + (ff // d) * d + sum(x.shape[1] for x in more)), BF)
    return pl.pallas_call(
        functools.partial(_mlp_backward, n=n, ff=ff, base=base, join=join is not None),
        grid=(t // BLOCK,),
        in_specs=[rows, rows, _whole(w.shape)] + [_whole(x.shape) for x in more],
        out_specs=[rows, _whole(g.shape)],
        out_shape=[jax.ShapeDtypeStruct((t, d), BF), g],
        scratch_shapes=[pltpu.VMEM((ff, d), BF), pltpu.VMEM((d, 2 * ff), F32), pltpu.VMEM((d, ff), F32)],
        compiler_params=_params(),
        cost_estimate=_cost(18 * t * d * ff, t * ff, [h, h, h, w, w]),
        name="mlp_backward",
    )(dy, h, w, *more)


def tables(tokens):
    half = HEAD // 2
    angle = jnp.arange(tokens, dtype=F32)[:, None] * THETA ** (-jnp.arange(half, dtype=F32) / half)
    cos, sin = jnp.cos(angle), jnp.sin(angle)
    return jnp.concatenate([cos, cos], -1), jnp.concatenate([-sin, sin], -1)


def _pack(*refs, layers):
    ws, outs = refs[:7], refs[7:]

    def attn(number, to, at):
        for w in ws[:3]:
            to[:, at : at + w.shape[2]] = w[number]
            at += w.shape[2]
        wo, d, r = ws[3], ws[3].shape[2], to.shape[0]
        half, rest = d // 2, wo.shape[1] - r
        to[:, at : at + d] = wo[number, :r, :]
        to[:rest, at + d : at + d + half] = wo[number, r:, :half]
        to[rest:, at + d : at + d + half] = wo[number, r:, half:]
        return at + d + half

    attn(0, outs[0], 0)
    for number in range(layers):
        to = outs[1 + number]
        at = attn(number + 1, to, 0) if number + 1 < layers else 0
        for w in ws[4:6]:
            to[:, at : at + w.shape[2]] = w[number]
            at += w.shape[2]
        wd, r = ws[6], to.shape[0]
        for q in range(0, wd.shape[1], r):
            to[:, at : at + wd.shape[2]] = wd[number, q : q + r, :]
            at += wd.shape[2]


def pack(weights):
    layers, r, ff = weights[4].shape
    d = weights[6].shape[2]
    first = sum(w.shape[2] for w in weights[:3]) + d + d // 2
    mlp = 2 * ff + weights[6].shape[1] // r * d
    widths = [first] + [mlp + (first if number + 1 < layers else 0) for number in range(layers)]
    return first, pl.pallas_call(
        functools.partial(_pack, layers=layers),
        out_shape=[jax.ShapeDtypeStruct((r, width), BF) for width in widths],
        name="pack",
    )(*weights)


def _greet(others):
    barrier = pltpu.get_barrier_semaphore()
    for other in others:
        pl.semaphore_signal(barrier, inc=1, device_id={"dp": other}, device_id_type=pl.DeviceIdType.MESH)
    pl.semaphore_wait(barrier, len(others))


def _send(source, target, sends, recvs, number, to):
    return pltpu.make_async_remote_copy(src_ref=source, dst_ref=target, send_sem=sends.at[number], recv_sem=recvs.at[number],
                                        device_id={"dp": to}, device_id_type=pl.DeviceIdType.MESH)


def _places(n):
    me = lax.axis_index("dp")
    chip, core = lax.div(me, 2), lax.rem(me, 2)
    chips = n // 2
    return me, core, chips, lambda away: 2 * lax.rem(chip + away + chips, chips) + core


def _gather(own_ref, all_ref, send_s, recv_s, pass_s, take_s, *, n):
    me, core, chips, at = _places(n)
    reach = chips // 2
    r = own_ref.shape[0]
    partner = me + 1 - 2 * core
    _greet([at(1), at(-1), partner])
    rows = lambda index, start=0, size=r: all_ref.at[pl.ds(pl.multiple_of(index * r + start, size), size), :]
    started = []

    def go(copy):
        copy.start()
        started.append(copy)

    def onward(side, hops):
        sign = 1 if side == 0 else -1
        index = at(-sign * hops)
        part = (side * (r // 2), r // 2) if hops == reach - 1 else (0, r)
        source = own_ref.at[pl.ds(*part), :] if hops == 0 else rows(index, *part)
        go(_send(source, rows(index, *part), send_s, recv_s, side * reach + hops, at(sign)))

    def arrived(side, hops):
        sign = 1 if side == 0 else -1
        index = at(-sign * hops)
        part = (side * (r // 2), r // 2) if hops == reach else (0, r)
        here = rows(index, *part)
        _send(here, here, send_s, recv_s, side * reach + hops - 1, at(sign)).wait_recv()
        return here

    for side in (0, 1):
        onward(side, 0)
    go(_send(own_ref, rows(me), pass_s, take_s, 2 * reach, partner))
    all_ref[pl.ds(pl.multiple_of(me * r, r), r), :] = own_ref[...]
    for hops in range(1, reach + 1):
        for side in (0, 1):
            here = arrived(side, hops)
            if hops < reach:
                onward(side, hops)
            go(_send(here, here, pass_s, take_s, side * reach + hops - 1, partner))
    for hops in range(1, reach + 1):
        for side in (0, 1):
            index = at(-hops if side == 0 else hops) + 1 - 2 * core
            part = (side * (r // 2), r // 2) if hops == reach else (0, r)
            _send(rows(index, *part), rows(index, *part), pass_s, take_s, side * reach + hops - 1, partner).wait_recv()
    _send(rows(partner), rows(partner), pass_s, take_s, 2 * reach, partner).wait_recv()
    for copy in started:
        copy.wait_send()


def gather(own, n):
    r, columns = own.shape
    dma = pltpu.SemaphoreType.DMA
    steps = n // 2 // 2
    return pl.pallas_call(
        functools.partial(_gather, n=n),
        out_shape=jax.ShapeDtypeStruct((n * r, columns), BF),
        in_specs=[pl.BlockSpec(memory_space=pltpu.VMEM)],
        out_specs=pl.BlockSpec(memory_space=pltpu.VMEM),
        scratch_shapes=[dma((2 * steps,)), dma((2 * steps,)), dma((2 * steps + 1,)), dma((2 * steps + 1,))],
        compiler_params=pltpu.CompilerParams(collective_id=0, has_side_effects=True),
        cost_estimate=pl.CostEstimate(flops=2 * 10**10, transcendentals=0, bytes_accessed=2 * n * r * columns),
        name="gather",
    )(own)


def _scatter(g_ref, out_ref, other_s, out_s, in_s, send_s, recv_s, pass_s, take_s, *, n):
    me, core, chips, at = _places(n)
    reach = chips // 2
    r, columns = out_ref.shape
    partner = me + 1 - 2 * core
    _greet([at(1), at(-1), partner])
    started = []

    def go(copy):
        copy.start()
        started.append(copy)

    order = [reach] + [k for m in range(reach - 1, 0, -1) for k in (m, chips - m)] + [0]
    swap = lambda k: _send(g_ref.at[pl.ds(pl.multiple_of((at(k) + 1 - 2 * core) * r, r), r), :], other_s.at[k], pass_s, take_s, k, partner)
    for k in order:
        go(swap(k))
    have = set()

    def term(k):
        if k not in have:
            swap(k).wait_recv()
            have.add(k)
        return g_ref[pl.ds(pl.multiple_of(at(k) * r, r), r), :].astype(F32) + other_s[k].astype(F32)

    half = r // 2
    for hop in range(reach):
        for side in (0, 1):
            slot = side * reach + hop
            sign = 1 if side == 0 else -1
            k = (sign * (reach - hop)) % chips
            mine = term(k)
            own = slice(side * half, (side + 1) * half)
            if hop == 0:
                out_s[slot, own, :] = mine[own].astype(BF)
                part = pl.ds(side * half, half)
                go(_send(out_s.at[slot, part, :], in_s.at[slot, part, :], send_s, recv_s, slot, at(sign)))
                continue
            before = slot - 1
            if hop == 1:
                part = pl.ds(side * half, half)
                _send(out_s.at[before, part, :], in_s.at[before, part, :], send_s, recv_s, before, at(sign)).wait_recv()
                rest = slice((1 - side) * half, (2 - side) * half)
                out_s[slot, own, :] = (mine[own] + in_s[before, own, :].astype(F32)).astype(BF)
                out_s[slot, rest, :] = mine[rest].astype(BF)
            else:
                _send(out_s.at[before], in_s.at[before], send_s, recv_s, before, at(sign)).wait_recv()
                out_s[slot] = (mine + in_s[before].astype(F32)).astype(BF)
            go(_send(out_s.at[slot], in_s.at[slot], send_s, recv_s, slot, at(sign)))
    total = term(0)
    for side in (0, 1):
        slot = side * reach + reach - 1
        _send(out_s.at[slot], in_s.at[slot], send_s, recv_s, slot, at(1)).wait_recv()
        total = total + in_s[slot].astype(F32)
    out_ref[...] = total.astype(BF)
    for copy in started:
        copy.wait_send()


def scatter(g, n):
    r, columns = g.shape[0] // n, g.shape[1]
    dma = pltpu.SemaphoreType.DMA
    chips = n // 2
    steps = chips // 2
    return pl.pallas_call(
        functools.partial(_scatter, n=n),
        out_shape=jax.ShapeDtypeStruct((r, columns), BF),
        in_specs=[pl.BlockSpec(memory_space=pltpu.VMEM)],
        out_specs=pl.BlockSpec(memory_space=pltpu.VMEM),
        scratch_shapes=[pltpu.VMEM((chips, r, columns), BF), pltpu.VMEM((2 * steps, r, columns), BF), pltpu.VMEM((2 * steps, r, columns), BF),
                        dma((2 * steps,)), dma((2 * steps,)), dma((chips,)), dma((chips,))],
        compiler_params=pltpu.CompilerParams(collective_id=1, has_side_effects=True),
        cost_estimate=pl.CostEstimate(flops=2 * 10**10, transcendentals=0, bytes_accessed=2 * g.size),
        name="scatter",
    )(g)


def _clip(*refs, n, count):
    gs, (out_ref, all_s, send_s, recv_s) = refs[:-4], refs[-4:]
    me = lax.axis_index("dp")
    others = [lax.rem(me + k, n) for k in range(1, n)]
    own = None
    for g in gs:
        for c in range(0, g.shape[1], 128):
            x = g[:, c : c + 128].astype(F32)
            own = x * x if own is None else own + x * x
    all_s[0] = own
    _greet(others)
    copies = [_send(all_s.at[0], all_s.at[k], send_s, recv_s, k - 1, others[k - 1]) for k in range(1, n)]
    for copy in copies:
        copy.start()
    for copy in copies:
        copy.wait_recv()
    total = all_s[0]
    for k in range(1, n):
        total = total + all_s[k]
    total = jnp.sum(jnp.sum(total, axis=0, keepdims=True), axis=1, keepdims=True)
    factor = jnp.minimum(1.0, 0.5 * lax.rsqrt(total / count + 1e-30))
    out_ref[...] = jnp.broadcast_to(factor, out_ref.shape)
    for copy in copies:
        copy.wait_send()


def clip(gs, n):
    r = gs[0].shape[0]
    dma = pltpu.SemaphoreType.DMA
    return pl.pallas_call(
        functools.partial(_clip, n=n, count=float(n * sum(g.size for g in gs))),
        out_shape=jax.ShapeDtypeStruct((8, 128), F32),
        in_specs=[pl.BlockSpec(memory_space=pltpu.VMEM)] * len(gs),
        out_specs=pl.BlockSpec(memory_space=pltpu.VMEM),
        scratch_shapes=[pltpu.VMEM((n, r, 128), F32), dma((n - 1,)), dma((n - 1,))],
        compiler_params=pltpu.CompilerParams(collective_id=2, has_side_effects=True),
        cost_estimate=pl.CostEstimate(flops=5 * 10**9, transcendentals=0, bytes_accessed=sum(2 * g.size for g in gs)),
        name="clip",
    )(*gs)


def unpack_attn(g, wq, wk, wv, wo):
    a, b, c = wq.shape[-1], wk.shape[-1], wv.shape[-1]
    d, rest = wo.shape[-1], wo.shape[-2] - g.shape[0]
    at = a + b + c
    tail = g[:, at + d :]
    return g[:, :a], g[:, a : a + b], g[:, a + b : at], jnp.concatenate([g[:, at : at + d], jnp.concatenate([tail[:rest], tail[rest:]], 1)], 0)


def unpack_mlp(g, ff, d):
    g = g[:, : 3 * ff]
    return g[:, :ff], g[:, ff : 2 * ff], jnp.concatenate([g[:, i : i + d] for i in range(2 * ff, g.shape[1], d)], 0)


def adamw(w, m, v, g):
    m = 0.9 * m + 0.1 * g
    v = 0.95 * v + 0.05 * g * g
    step = m * lax.rsqrt(v + 1e-8) + 0.1 * w
    return (w - 0.02 * step).astype(BF), m, v


def solution(mesh):
    n = mesh.shape["dp"]

    def gathered(x):
        return lax.all_gather(x, "dp", axis=0, tiled=True)

    def scattered(x):
        return lax.psum_scatter(x, "dp", scatter_dimension=0, tiled=True)

    def step(x, dy, *arrays):
        weights, m, v = (arrays[i : i + 7] for i in (0, 7, 14))
        layers, ff = weights[0].shape[0], weights[4].shape[2]
        heads = weights[0].shape[2] // HEAD
        d = x.shape[2]
        cos, sin = tables(x.shape[1])
        first, (head, *packed) = pack(weights)
        fetched, w_attn = [gathered(packed[0])], [gather(head, n)]
        base = [first] * (layers - 1) + [0]
        h, kept = x[0], []
        for number in range(layers):
            q, k, v_, o, lse, mid = attn_forward(h, w_attn[number], cos, sin, n, heads)
            kept.append((h, q, k, v_, o, lse, mid))
            if number < layers - 1:
                w_attn.append(fetched[number])
                fetched.append(gathered(lax.optimization_barrier((packed[number + 1], mid))[0]))
                h = mlp_forward(mid, fetched[number], n, ff, base[number])
        by_h, summed, g_attn = dy[0], [None] * layers, None
        for number in reversed(range(layers)):
            h, q, k, v_, o, lse, mid = kept[number]
            by_mid, g = mlp_backward(by_h, mid, fetched[number], n, ff, base[number], g_attn)
            if number < layers - 1:
                g = lax.optimization_barrier((g, summed[number + 1]))[0]
            summed[number] = scattered(g)
            by_h, g_attn = attn_backward(by_mid, h, q, k, v_, o, lse, w_attn[number], cos, sin, n, number > 0)
        last = scatter(g_attn, n)
        factor = clip([last, *summed], n)[0, 0]
        mine = []
        for number in range(layers):
            attn = last if number == 0 else summed[number - 1][:, -first:]
            mine.append([*unpack_attn(attn, *weights[:4]), *unpack_mlp(summed[number], ff, d)])
        gradients = [jnp.stack([mine[number][i] for number in range(layers)]).astype(F32) * factor for i in range(7)]
        new = [adamw(w.astype(F32), m, v, g) for w, m, v, g in zip(weights, m, v, gradients, strict=True)]
        return tuple(one[which] for which in range(3) for one in new)

    states, cut = P(("rep", "dp"), None, None), P(None, "dp", None)
    return jax.shard_map(
        step,
        mesh=mesh,
        in_specs=(states, states) + (cut,) * 21,
        out_specs=(P("rep", "dp", None),) * 21,
        check_vma=False,
    )
```

```python
import functools

import jax
import jax.numpy as jnp
from jax import lax
from jax.experimental import pallas as pl
from jax.experimental.pallas import tpu as pltpu
from jax.sharding import PartitionSpec as P

NEG = -1e30
LOG2E = 1.4426950408889634
HEAD = 128
THETA = 10000
NAMES = ("wq", "wk", "wv", "wo", "w_gate", "w_up", "w_down")
BLOCK = 512
COARSE = 64
BF, F32 = jnp.bfloat16, jnp.float32
MIB = 58
MLP_BLOCK = 512


def _dot(a, b, ca=1, cb=0):
    return lax.dot_general(a, b, (((ca,), (cb,)), ((), ())), preferred_element_type=F32)


def _dot_t(a, b):
    return _dot(a, b, 1, 1)


def _lanes(m):
    return slice(m * HEAD, m * HEAD + HEAD)


def _sign(side):
    return 1 - 2 * side


def _scale(x):
    return lax.rsqrt(jnp.mean(x * x, -1, keepdims=True) + 1e-6)


def _norm_back(x, r, d):
    y = x * r
    return r * (d - y * jnp.mean(d * y, -1, keepdims=True))


def _turn(t, cos, sin, back=False):
    t = t.astype(F32)
    other = pltpu.roll(t, HEAD // 2, 1) * sin
    return (t * cos - other if back else t * cos + other).astype(BF)


def _unpack_wo(w_ref, wo_s, at, n):
    d = w_ref.shape[0]
    r, each, half = d // n, wo_s.shape[0] // n, d // 2
    rest = each - r
    for i in range(n):
        wo_s[i * each : i * each + r, :] = w_ref[i * r : i * r + r, at : at + d]
        wo_s[i * each + r : i * each + each, :half] = w_ref[i * r : i * r + rest, at + d : at + d + half]
        wo_s[i * each + r : i * each + each, half:] = w_ref[i * r + rest : i * r + r, at + d : at + d + half]


def _gap(b):
    return lax.broadcasted_iota(jnp.int32, (b, b), 1) - lax.broadcasted_iota(jnp.int32, (b, b), 0)


def _attn_forward(h_ref, w_ref, cos_ref, sin_ref, q_ref, k_ref, v_ref, o_ref, lse_ref, k_s, vt_s, top_s, mix_s, gap_s, *, heads):
    i = pl.program_id(0)
    b, hd = h_ref.shape[0], heads * HEAD
    e = HEAD**-0.5 * LOG2E

    @pl.when(i == 0)
    def _():
        gap_s[...] = _gap(b)
        vt_s[HEAD:, :] = jnp.ones((vt_s.shape[0] - HEAD, vt_s.shape[1]), BF)

    here = pl.ds(pl.multiple_of(i * b, b), b)
    x = h_ref[...].astype(F32)
    a = (x * _scale(x)).astype(BF)
    cos, sin = cos_ref[...], sin_ref[...]
    kv = _dot(a, w_ref[:, hd : hd + 2 * HEAD]).astype(BF)
    k = _turn(kv[:, :HEAD], cos, sin)
    v = kv[:, HEAD:]
    k_ref[...] = k
    v_ref[...] = v
    k_s[here, :] = k
    vt_s[:HEAD, here] = v.T
    for m in range(heads):
        at = _lanes(m)
        q_ref[:, at] = _turn(_dot(a, w_ref[:, at]).astype(BF), cos, sin)
    top_s[...] = jnp.full(top_s.shape, NEG, F32)
    mix_s[...] = jnp.zeros(mix_s.shape, F32)

    def block(start, keys, cut, masked):
        there = pl.ds(pl.multiple_of(start, keys), keys)
        kj, vj = k_s[there, :], vt_s[:, there]
        scores = [_dot_t(kj, q_ref[cut:, _lanes(m)]) for m in range(heads)]
        ps, keeps = [], []
        for m, s in enumerate(scores):
            if masked:
                s = jnp.where(gap_s[:keys, : b - cut] >= 0, s, 2 * NEG)
            old = top_s[m : m + 1, cut:]
            top = jnp.maximum(old, s.max(axis=0, keepdims=True))
            top_s[m : m + 1, cut:] = top
            ps.append(jnp.exp2((s - top) * e).astype(BF))
            keeps.append(jnp.exp2((old - top) * e))
        for m in range(heads):
            mix_s[m, :, cut:] = mix_s[m, :, cut:] * keeps[m] + _dot(vj, ps[m])

    lax.fori_loop(0, i, lambda j, _: block(j * b, b, 0, False), None)
    block(i * b, b // 2, 0, True)
    block(i * b + b // 2, b // 2, b // 2, True)
    for m in range(heads):
        total = mix_s[m, HEAD : HEAD + 1, :]
        o_ref[:, _lanes(m)] = (mix_s[m, :HEAD, :] * (1 / total)).T.astype(BF)
        lse_ref[m : m + 1, :] = top_s[m : m + 1, :] * e + jnp.log(total) * LOG2E
    lse_ref[heads:, :] = jnp.zeros((lse_ref.shape[0] - heads, b), F32)


def _attn_backward(dm_ref, do_ref, h_ref, q_ref, k_ref, v_ref, o_ref, lse_ref, w_ref, cos_ref, sin_ref, *refs, heads, need):
    dh_ref, refs = (refs[0], refs[1:]) if need else (None, refs)
    g_ref, dk_s, dv_s, dq_s, wqkv_s, kt_s, gap_s = refs
    step, blocks = pl.program_id(0), pl.num_programs(0)
    i = blocks - 1 - step
    b = h_ref.shape[0]
    scale = HEAD**-0.5
    e = scale * LOG2E

    @pl.when(step == 0)
    def _():
        gap_s[...] = _gap(b)
        dk_s[...] = jnp.zeros(dk_s.shape, F32)
        dv_s[...] = jnp.zeros(dv_s.shape, F32)
        wqkv_s[...] = jnp.zeros(wqkv_s.shape, F32)
        kt_s[...] = k_ref[...].T

    dq_s[...] = jnp.zeros(dq_s.shape, F32)
    deltas = []
    for m in range(heads):
        at = _lanes(m)
        deltas.append((do_ref[:, at].astype(F32) * o_ref[:, at].astype(F32)).T.sum(axis=0, keepdims=True))

    def block(start, keys, cut, masked):
        there = pl.ds(pl.multiple_of(start, keys), keys)
        kj, vj, ktj = k_ref[there, :], v_ref[there, :], kt_s[:, there]
        lanes = [_lanes(m) for m in range(heads)]
        scores = [_dot_t(kj, q_ref[cut:, at]) for at in lanes]
        dps = [_dot_t(vj, do_ref[cut:, at]) for at in lanes]
        for m, at in enumerate(lanes):
            p = jnp.exp2(scores[m] * e - lse_ref[m : m + 1, cut:])
            if masked:
                p = jnp.where(gap_s[:keys, : b - cut] >= 0, p, 0.0)
            ds = (p * (dps[m] - deltas[m][:, cut:])).astype(BF)
            dv_s[there, :] += _dot(p.astype(BF), do_ref[cut:, at])
            dk_s[there, :] += _dot(ds, q_ref[cut:, at])
            dq_s[m, :, cut:] += _dot(ktj, ds)

    lax.fori_loop(0, i, lambda j, _: block(j * b, b, 0, False), None)
    block(i * b, b // 2, 0, True)
    block(i * b + b // 2, b // 2, b // 2, True)

    here = pl.ds(pl.multiple_of(i * b, b), b)
    cos, sin = cos_ref[...], sin_ref[...]
    parts = [_turn((dq_s[m] * scale).T.astype(BF), cos, sin, True) for m in range(heads)]
    parts += [_turn((dk_s[here, :] * scale).astype(BF), cos, sin, True), dv_s[here, :].astype(BF)]
    dqkv = jnp.concatenate(parts, axis=1)
    x = h_ref[...].astype(F32)
    r = _scale(x)
    wqkv_s[...] += _dot((x * r).astype(BF), dqkv, 0, 0)
    if need:
        da = _dot_t(dqkv, w_ref[...]).astype(BF).astype(F32)
        dh_ref[...] = (dm_ref[...].astype(F32) + _norm_back(x, r, da)).astype(BF)

    @pl.when(step == blocks - 1)
    def _():
        g_ref[...] = wqkv_s[...].astype(BF)


def _sigmoid(x):
    return 0.5 + 0.5 * jnp.tanh(0.5 * x)


def _sigmoid(x):
    return 0.5 + 0.5 * jnp.tanh(0.5 * x)


class _Weights:
    def __init__(self, w_ref, base, w_s, wo_s, wd_s, sems, n, ff):
        d, (hd, _) = w_s.shape[0], wo_s.shape
        self.n, self.ff, self.d, self.hd, self.w_s, self.wo_s, self.wd_s = n, ff, d, hd, w_s, wo_s, wd_s
        self.rows = d * d // ff
        moves = [[(slice(0, d), slice(0, hd))]]
        for c in range(ff // d):
            own = slice(c * self.rows, (c + 1) * self.rows)
            moves.append([(slice(0, d), slice(hd + at, hd + at + d)) for at in (c * d, ff + c * d)] + [(own, slice(hd + 2 * ff, hd + 2 * ff + ff // d * d))])
        self.copies = [[pltpu.make_async_copy(w_ref.at[a, base + b.start : base + b.stop], w_s.at[a, b], sems.at[i, j]) for j, (a, b) in enumerate(m)]
                       for i, m in enumerate(moves)]

    def start(self):
        for piece in self.copies:
            for copy in piece:
                copy.start()

    def ready(self, piece):
        for copy in self.copies[piece]:
            copy.wait()
        d, n = self.d, self.n
        if piece == 0:
            _unpack_wo(self.w_s, self.wo_s, 0, n)
            return
        r, each = d // n, self.ff // n
        for i in range((piece - 1) * d // each, piece * d // each):
            for q in range(each // r):
                at = self.hd + 2 * self.ff + q * d
                self.wd_s[i * each + q * r : i * each + (q + 1) * r, :] = self.w_s[i * r : (i + 1) * r, at : at + d]


def _sigmoid(x):
    return 0.5 + 0.5 * jnp.tanh(0.5 * x)


def _mlp_forward(h_ref, o_ref, w_ref, y_ref, w_s, wo_s, wd_s, sems, *, n, ff, base):
    d, (hd, _) = h_ref.shape[1], wo_s.shape
    weights = _Weights(w_ref, base, w_s, wo_s, wd_s, sems, n, ff)

    def block(fresh):
        if fresh:
            weights.start()
            weights.ready(0)
        x = (h_ref[...].astype(F32) + _dot(o_ref[...], wo_s[...]).astype(BF).astype(F32)).astype(BF).astype(F32)
        a = (x * _scale(x)).astype(BF)
        y = None
        for c in range(0, ff, d):
            if fresh:
                weights.ready(1 + c // d)
            gate, up = (_dot(a, w_s[:, at : at + d]) for at in (hd + c, hd + ff + c))
            part = _dot((gate * _sigmoid(gate) * up).astype(BF), wd_s[c : c + d, :])
            y = part if y is None else y + part
        y_ref[...] = (x + y.astype(BF).astype(F32)).astype(BF)

    pl.when(pl.program_id(0) == 0)(lambda: block(True))
    pl.when(pl.program_id(0) > 0)(lambda: block(False))


def _mlp_backward(dy_ref, h_ref, o_ref, w_ref, *refs, n, ff, base, join):
    g_in, refs = (refs[0], refs[1:]) if join else (None, refs)
    dm_ref, do_ref, g_ref, w_s, wo_s, wd_s, dgu_s, dwd_s, dwo_s, g_s, sems, out_sems = refs[:12]
    d, (hd, _) = h_ref.shape[1], wo_s.shape
    tail_at = hd + 2 * ff
    step, last = pl.program_id(0), pl.num_programs(0) - 1
    weights = _Weights(w_ref, base, w_s, wo_s, wd_s, sems, n, ff)
    fresh, final = step == 0, step == last
    rows, each, chunks = d // n, ff // n, ff // d
    pieces = [[(slice(0, d), slice(0, hd))]]
    for c in range(chunks):
        own = slice(c * d // chunks, (c * d + d) // chunks)
        pieces.append([(slice(0, d), slice(hd + at, hd + at + d)) for at in (c * d, ff + c * d)] + [(own, slice(tail_at, tail_at + chunks * d))])
    outs = [[pltpu.make_async_copy(g_s.at[a, b], g_ref.at[a, b], out_sems.at[i, j]) for j, (a, b) in enumerate(m)] for i, m in enumerate(pieces)]
    if join:
        behind = slice(tail_at + chunks * d, g_ref.shape[1])
        outs.append([pltpu.make_async_copy(g_in, g_ref.at[:, behind], out_sems.at[chunks + 1, 0])])

    def block(fresh):
        if fresh:
            weights.start()
            dgu_s[...] = jnp.zeros(dgu_s.shape, F32)
            dwd_s[...] = jnp.zeros(dwd_s.shape, F32)
            dwo_s[...] = jnp.zeros(dwo_s.shape, F32)
            weights.ready(0)
        o = o_ref[...]
        x = (h_ref[...].astype(F32) + _dot(o, wo_s[...]).astype(BF).astype(F32)).astype(BF).astype(F32)
        r = _scale(x)
        a = (x * r).astype(BF)
        dy = dy_ref[...]
        at, dyt = a.T, dy.T
        da = None
        for c in range(0, ff, d):
            if fresh:
                weights.ready(1 + c // d)
            wg, wu = (w_s[:, m : m + d] for m in (hd + c, hd + ff + c))
            gate, up = _dot(a, wg), _dot(a, wu)
            du = _dot_t(dy, wd_s[c : c + d, :]).astype(BF).astype(F32)
            s = _sigmoid(gate)
            silu = gate * s
            u = (silu * up).astype(BF)
            dup = (du * silu).astype(BF)
            dgate = (du * up * (s * (1 + gate * (1 - s)))).astype(BF)
            part = _dot_t(dgate, wg) + _dot_t(dup, wu)
            da = part if da is None else da + part
            dgu_s[:, c : c + d] += _dot(at, dgate)
            dgu_s[:, ff + c : ff + c + d] += _dot(at, dup)
            dwd_s[:, c : c + d] += _dot(dyt, u)
        da = da.astype(BF).astype(F32)
        dm = (dy.astype(F32) + _norm_back(x, r, da)).astype(BF)
        dm_ref[...] = dm
        do_ref[...] = _dot_t(dm, wo_s[...]).astype(BF)
        dwo_s[...] += _dot(o, dm, 0, 0)

    pl.when(fresh)(lambda: block(True))
    pl.when(step > 0)(lambda: block(False))

    @pl.when(final)
    def _():
        if join:
            outs[-1][0].start()
        for c in range(0, ff, d):
            for m in (c, ff + c):
                g_s[:, hd + m : hd + m + d] = dgu_s[:, m : m + d].astype(BF)
            for m in range(c // each, (c + d) // each):
                own = dwd_s[:, m * each : m * each + each].T.astype(BF)
                for q in range(each // rows):
                    at_q = tail_at + q * d
                    g_s[m * rows : m * rows + rows, at_q : at_q + d] = own[q * rows : q * rows + rows, :]
            for copy in outs[1 + c // d]:
                copy.start()
        own, half = hd // n, d // 2
        rest = own - rows
        for m in range(n):
            g_s[m * rows : m * rows + rows, :d] = dwo_s[m * own : m * own + rows, :].astype(BF)
            tail = dwo_s[m * own + rows : m * own + own, :].astype(BF)
            g_s[m * rows : m * rows + rest, d:hd] = tail[:, :half]
            g_s[m * rows + rest : m * rows + rows, d:hd] = tail[:, half:]
        outs[0][0].start()
        for piece in outs:
            for copy in piece:
                copy.wait()


def _whole(shape):
    return pl.BlockSpec(shape, lambda i: (0,) * len(shape), pipeline_mode=pl.Buffered(1))


def _params():
    return pltpu.CompilerParams(dimension_semantics=("arbitrary",), vmem_limit_bytes=MIB * 2**20)


def _cost(flops, exps, arrays):
    return pl.CostEstimate(flops=flops, transcendentals=exps, bytes_accessed=sum(a.size * a.dtype.itemsize for a in arrays))


def attn_forward(h, w, cos, sin, heads):
    t, d = h.shape
    b, hd = BLOCK, heads * HEAD
    rows = lambda width: pl.BlockSpec((b, width), lambda i: (i, 0))
    shape = jax.ShapeDtypeStruct
    wide = hd + 2 * HEAD
    return pl.pallas_call(
        functools.partial(_attn_forward, heads=heads),
        grid=(t // b,),
        in_specs=[rows(d), _whole((d, wide)), rows(HEAD), rows(HEAD)],
        out_specs=[rows(hd), rows(HEAD), rows(HEAD), rows(hd), pl.BlockSpec((8, b), lambda i: (0, i))],
        out_shape=[shape((t, hd), BF), shape((t, HEAD), BF), shape((t, HEAD), BF), shape((t, hd), BF), shape((8, t), F32)],
        scratch_shapes=[pltpu.VMEM((t, HEAD), BF), pltpu.VMEM((HEAD + 16, t), BF), pltpu.VMEM((8, b), F32), pltpu.VMEM((heads, HEAD + 16, b), F32),
                        pltpu.VMEM((b, b), jnp.int32)],
        compiler_params=_params(),
        cost_estimate=_cost(2 * t * d * wide + 4 * heads * t * t * HEAD, heads * t * t, [h, h, h, h, h]),
        name="attn_forward",
    )(h, w, cos, sin)


def attn_backward(dm, do, h, q, k, v, o, lse, w, cos, sin, need):
    t, d = h.shape
    b, hd = BLOCK, q.shape[1]
    heads = hd // HEAD
    wide = hd + 2 * HEAD
    last = t // b - 1
    rows = lambda width: pl.BlockSpec((b, width), lambda i: (last - i, 0))
    given = [dm, do, h, q, k, v, o, lse, w, cos, sin]
    g = jax.ShapeDtypeStruct((d, wide), BF)
    outs = ([(jax.ShapeDtypeStruct((t, d), BF), rows(d))] if need else []) + [(g, _whole(g.shape))]
    got = pl.pallas_call(
        functools.partial(_attn_backward, heads=heads, need=need),
        grid=(t // b,),
        in_specs=[rows(d), rows(hd), rows(d), rows(hd), _whole(k.shape), _whole(v.shape), rows(hd), pl.BlockSpec((8, b), lambda i: (0, last - i)),
                  _whole((d, wide)), rows(HEAD), rows(HEAD)],
        out_specs=[spec for _, spec in outs],
        out_shape=[shape for shape, _ in outs],
        scratch_shapes=[pltpu.VMEM((t, HEAD), F32), pltpu.VMEM((t, HEAD), F32), pltpu.VMEM((heads, HEAD, b), F32),
                        pltpu.VMEM((d, wide), F32), pltpu.VMEM((HEAD, t), BF), pltpu.VMEM((b, b), jnp.int32)],
        compiler_params=_params(),
        cost_estimate=_cost(4 * t * d * wide + 10 * heads * t * t * HEAD, heads * t * t, given[:-3]),
        name="attn_backward",
    )(*given)
    return got if need else (None, got[0])


def _mlp_scratch(d, hd, ff):
    dma = pltpu.SemaphoreType.DMA
    return [pltpu.VMEM((d, hd + 2 * ff + ff // d * d), BF), pltpu.VMEM((hd, d), BF), pltpu.VMEM((ff, d), BF)], dma((ff // d + 1, 3)), dma((ff // d + 2, 3))


def mlp_forward(h, o, w, n, ff, base):
    t, d = h.shape
    hd = o.shape[1]
    b = MLP_BLOCK
    rows = lambda width: pl.BlockSpec((b, width), lambda i: (i, 0))
    vmem, sems, _ = _mlp_scratch(d, hd, ff)
    return pl.pallas_call(
        functools.partial(_mlp_forward, n=n, ff=ff, base=base),
        grid=(t // b,),
        in_specs=[rows(d), rows(hd), pl.BlockSpec(memory_space=pl.ANY)],
        out_specs=rows(d),
        out_shape=jax.ShapeDtypeStruct((t, d), BF),
        scratch_shapes=[*vmem, sems],
        compiler_params=_params(),
        cost_estimate=_cost(2 * t * (3 * ff + hd) * d, t * ff, [h, h, o, w]),
        name="mlp_forward",
    )(h, o, w)


def mlp_backward(dy, h, o, w, n, ff, base, join):
    t, d = h.shape
    hd = o.shape[1]
    b = MLP_BLOCK
    rows = lambda width: pl.BlockSpec((b, width), lambda i: (i, 0))
    more = [] if join is None else [join]
    g = jax.ShapeDtypeStruct((d, hd + 2 * ff + (ff // d) * d + sum(x.shape[1] for x in more)), BF)
    vmem, sems, out_sems = _mlp_scratch(d, hd, ff)
    return pl.pallas_call(
        functools.partial(_mlp_backward, n=n, ff=ff, base=base, join=join is not None),
        grid=(t // b,),
        in_specs=[rows(d), rows(d), rows(hd), pl.BlockSpec(memory_space=pl.ANY)] + [_whole(x.shape) for x in more],
        out_specs=[rows(d), rows(hd), pl.BlockSpec(memory_space=pl.ANY)],
        out_shape=[jax.ShapeDtypeStruct((t, d), BF), jax.ShapeDtypeStruct((t, hd), BF), g],
        scratch_shapes=[*vmem, pltpu.VMEM((d, 2 * ff), F32), pltpu.VMEM((d, ff), F32), pltpu.VMEM((hd, d), F32), vmem[0], sems, out_sems],
        compiler_params=_params(),
        cost_estimate=_cost(18 * t * d * ff + 6 * t * hd * d, t * ff, [h, h, h, o, o, w, w]),
        name="mlp_backward",
    )(dy, h, o, w, *more)


def tables(tokens):
    half = HEAD // 2
    power = THETA ** (-jnp.arange(half, dtype=F32) / half)
    power = jnp.concatenate([power, power])
    many = jnp.arange(0, tokens, COARSE, dtype=F32)[:, None] * power
    few = jnp.arange(COARSE, dtype=F32)[:, None] * power
    return jnp.cos(many), jnp.sin(many), jnp.cos(few), jnp.sin(few)


def _pack(*refs, layers):
    ws, outs = refs[:7], refs[7:]

    def side_by_side(number, which, to, at):
        for w in which:
            to[:, at : at + w.shape[2]] = w[number]
            at += w.shape[2]
        return at

    side_by_side(0, ws[:3], outs[0], 0)
    for number in range(layers):
        to = outs[1 + number]
        at = side_by_side(number + 1, ws[:3], to, 0) if number + 1 < layers else 0
        wo, d, r = ws[3], ws[3].shape[2], to.shape[0]
        half, rest = d // 2, wo.shape[1] - r
        to[:, at : at + d] = wo[number, :r, :]
        to[:rest, at + d : at + d + half] = wo[number, r:, :half]
        to[rest:, at + d : at + d + half] = wo[number, r:, half:]
        at = side_by_side(number, ws[4:6], to, at + d + half)
        wd = ws[6]
        for q in range(0, wd.shape[1], r):
            to[:, at : at + d] = wd[number, q : q + r, :]
            at += d


def pack(weights):
    layers, r, ff = weights[4].shape
    d = weights[6].shape[2]
    first = sum(w.shape[2] for w in weights[:3])
    rest = d + d // 2 + 2 * ff + weights[6].shape[1] // r * d
    widths = [first] + [rest + (first if number + 1 < layers else 0) for number in range(layers)]
    return first, pl.pallas_call(
        functools.partial(_pack, layers=layers),
        out_shape=[jax.ShapeDtypeStruct((r, width), BF) for width in widths],
        name="pack",
    )(*weights)


def _greet(others):
    barrier = pltpu.get_barrier_semaphore()
    for other in others:
        pl.semaphore_signal(barrier, inc=1, device_id={"dp": other}, device_id_type=pl.DeviceIdType.MESH)
    return lambda: pl.semaphore_wait(barrier, len(others))


def _send(source, target, sends, recvs, number, to):
    return pltpu.make_async_remote_copy(src_ref=source, dst_ref=target, send_sem=sends.at[number], recv_sem=recvs.at[number],
                                        device_id={"dp": to}, device_id_type=pl.DeviceIdType.MESH)


def _places(n):
    me = lax.axis_index("dp")
    chip, core = lax.div(me, 2), lax.rem(me, 2)
    chips = n // 2
    return me, core, chips, lambda away: 2 * lax.rem(chip + away + chips, chips) + core


def _gather(own_ref, cm_ref, sm_ref, cf_ref, sf_ref, all_ref, cos_ref, sin_ref, send_s, recv_s, pass_s, take_s, *, n):
    me, core, chips, at = _places(n)
    reach = chips // 2
    r = own_ref.shape[0]
    partner = me + 1 - 2 * core
    _greet([at(1), at(-1), partner])()
    rows = lambda index, start=0, size=r: all_ref.at[pl.ds(pl.multiple_of(index * r + start, size), size), :]
    piece = lambda side, cut: (side * (r // 2), r // 2) if cut else (0, r)
    started = []

    def go(copy):
        copy.start()
        started.append(copy)

    def onward(side, hops):
        sign = _sign(side)
        index = at(-sign * hops)
        part = piece(side, hops + 1 == reach)
        source = own_ref.at[pl.ds(*part), :] if hops == 0 else rows(index, *part)
        go(_send(source, rows(index, *part), send_s, recv_s, side * reach + hops, at(sign)))

    def arrived(side, hops):
        sign = _sign(side)
        index = at(-sign * hops)
        part = piece(side, hops == reach)
        here = rows(index, *part)
        _send(here, here, send_s, recv_s, side * reach + hops - 1, at(sign)).wait_recv()
        return here

    for side in (0, 1):
        onward(side, 0)
    go(_send(own_ref, rows(me), pass_s, take_s, 2 * reach, partner))
    all_ref[pl.ds(pl.multiple_of(me * r, r), r), :] = own_ref[...]
    cf, sf = cf_ref[...], sf_ref[...]
    sign = jnp.where(lax.broadcasted_iota(jnp.int32, cf.shape, 1) < HEAD // 2, -1.0, 1.0)
    for m in range(cm_ref.shape[0]):
        cm, sm = cm_ref[m : m + 1, :], sm_ref[m : m + 1, :]
        cos_ref[m * COARSE : m * COARSE + COARSE, :] = cm * cf - sm * sf
        sin_ref[m * COARSE : m * COARSE + COARSE, :] = (sm * cf + cm * sf) * sign
    for hops in range(1, reach + 1):
        for side in (0, 1):
            here = arrived(side, hops)
            if hops < reach:
                onward(side, hops)
            go(_send(here, here, pass_s, take_s, side * reach + hops - 1, partner))
    for hops in range(1, reach + 1):
        for side in (0, 1):
            index = at(-_sign(side) * hops) + partner - me
            part = piece(side, hops == reach)
            _send(rows(index, *part), rows(index, *part), pass_s, take_s, side * reach + hops - 1, partner).wait_recv()
    _send(rows(partner), rows(partner), pass_s, take_s, 2 * reach, partner).wait_recv()
    for copy in started:
        copy.wait_send()


def gather(own, parts, n, tokens):
    r, columns = own.shape
    dma = pltpu.SemaphoreType.DMA
    steps = n // 2 // 2
    return pl.pallas_call(
        functools.partial(_gather, n=n),
        out_shape=[jax.ShapeDtypeStruct((n * r, columns), BF)] + [jax.ShapeDtypeStruct((tokens, HEAD), F32)] * 2,
        in_specs=[pl.BlockSpec(memory_space=pltpu.VMEM)] * 5,
        out_specs=[pl.BlockSpec(memory_space=pltpu.VMEM)] * 3,
        scratch_shapes=[dma((2 * steps,)), dma((2 * steps,)), dma((2 * steps + 1,)), dma((2 * steps + 1,))],
        compiler_params=pltpu.CompilerParams(collective_id=0, has_side_effects=True),
        cost_estimate=pl.CostEstimate(flops=2 * 10**10, transcendentals=0, bytes_accessed=2 * n * r * columns),
        name="gather",
    )(own, *parts)


def _scatter(g_ref, out_ref, other_s, out_s, in_s, send_s, recv_s, pass_s, take_s, *, n):
    me, core, chips, at = _places(n)
    reach = chips // 2
    r, columns = out_ref.shape
    partner = me + 1 - 2 * core
    _greet([at(1), at(-1), partner])()
    started = []

    def go(copy):
        copy.start()
        started.append(copy)

    order = [reach] + [k for m in range(reach - 1, 0, -1) for k in (m, chips - m)] + [0]
    swap = lambda k: _send(g_ref.at[pl.ds(pl.multiple_of((at(k) + 1 - 2 * core) * r, r), r), :], other_s.at[k], pass_s, take_s, k, partner)
    for k in order:
        go(swap(k))
    have = set()

    def term(k):
        if k not in have:
            swap(k).wait_recv()
            have.add(k)
        return g_ref[pl.ds(pl.multiple_of(at(k) * r, r), r), :].astype(F32) + other_s[k].astype(F32)

    half = r // 2
    for hop in range(reach):
        for side in (0, 1):
            slot = side * reach + hop
            sign = _sign(side)
            k = (sign * (reach - hop)) % chips
            mine = term(k)
            own = slice(side * half, side * half + half)
            if hop == 0:
                out_s[slot, own, :] = mine[own].astype(BF)
                part = pl.ds(side * half, half)
                go(_send(out_s.at[slot, part, :], in_s.at[slot, part, :], send_s, recv_s, slot, at(sign)))
                continue
            before = slot - 1
            if hop == 1:
                part = pl.ds(side * half, half)
                _send(out_s.at[before, part, :], in_s.at[before, part, :], send_s, recv_s, before, at(sign)).wait_recv()
                rest = slice(half - side * half, r - side * half)
                out_s[slot, own, :] = (mine[own] + in_s[before, own, :].astype(F32)).astype(BF)
                out_s[slot, rest, :] = mine[rest].astype(BF)
            else:
                _send(out_s.at[before], in_s.at[before], send_s, recv_s, before, at(sign)).wait_recv()
                out_s[slot] = (mine + in_s[before].astype(F32)).astype(BF)
            go(_send(out_s.at[slot], in_s.at[slot], send_s, recv_s, slot, at(sign)))
    total = term(0)
    for side in (0, 1):
        slot = side * reach + reach - 1
        _send(out_s.at[slot], in_s.at[slot], send_s, recv_s, slot, at(1)).wait_recv()
        total = total + in_s[slot].astype(F32)
    out_ref[...] = total.astype(BF)
    for copy in started:
        copy.wait_send()


def scatter(g, n):
    r, columns = g.shape[0] // n, g.shape[1]
    dma = pltpu.SemaphoreType.DMA
    chips = n // 2
    steps = chips // 2
    return pl.pallas_call(
        functools.partial(_scatter, n=n),
        out_shape=jax.ShapeDtypeStruct((r, columns), BF),
        in_specs=[pl.BlockSpec(memory_space=pltpu.VMEM)],
        out_specs=pl.BlockSpec(memory_space=pltpu.VMEM),
        scratch_shapes=[pltpu.VMEM((chips, r, columns), BF), pltpu.VMEM((2 * steps, r, columns), BF), pltpu.VMEM((2 * steps, r, columns), BF),
                        dma((2 * steps,)), dma((2 * steps,)), dma((chips,)), dma((chips,))],
        compiler_params=pltpu.CompilerParams(collective_id=1, has_side_effects=True),
        cost_estimate=pl.CostEstimate(flops=2 * 10**10, transcendentals=0, bytes_accessed=2 * g.size),
        name="scatter",
    )(g)


def _clip(*refs, n, count):
    gs, (out_ref, all_s, send_s, recv_s) = refs[:-4], refs[-4:]
    me = lax.axis_index("dp")
    others = [lax.rem(me + k, n) for k in range(1, n)]
    arrive = _greet(others)
    own = None
    for g in gs:
        for c in range(0, g.shape[1], 128):
            x = g[:, c : c + 128].astype(F32)
            own = x * x if own is None else own + x * x
    all_s[0] = sum(own[m : m + 8] for m in range(8, own.shape[0], 8)) + own[:8]
    arrive()
    copies = [_send(all_s.at[0], all_s.at[k], send_s, recv_s, k - 1, others[k - 1]) for k in range(1, n)]
    for copy in copies:
        copy.start()
    for copy in copies:
        copy.wait_recv()
    total = all_s[0]
    for k in range(1, n):
        total = total + all_s[k]
    total = jnp.sum(jnp.sum(total, axis=0, keepdims=True), axis=1, keepdims=True)
    factor = jnp.minimum(1.0, 0.5 * lax.rsqrt(total / count + 1e-30))
    out_ref[...] = jnp.broadcast_to(factor, out_ref.shape)
    for copy in copies:
        copy.wait_send()


def clip(gs, n):
    dma = pltpu.SemaphoreType.DMA
    return pl.pallas_call(
        functools.partial(_clip, n=n, count=float(n * sum(g.size for g in gs))),
        out_shape=jax.ShapeDtypeStruct((8, 128), F32),
        in_specs=[pl.BlockSpec(memory_space=pltpu.VMEM)] * len(gs),
        out_specs=pl.BlockSpec(memory_space=pltpu.VMEM),
        scratch_shapes=[pltpu.VMEM((n, 8, 128), F32), dma((n - 1,)), dma((n - 1,))],
        compiler_params=pltpu.CompilerParams(collective_id=2, has_side_effects=True),
        cost_estimate=pl.CostEstimate(flops=5 * 10**9, transcendentals=0, bytes_accessed=sum(2 * g.size for g in gs)),
        name="clip",
    )(*gs)


def _adam(*refs, first):
    f_ref, head_ref, refs = refs[0], refs[1], refs[2:]
    kinds = len(NAMES)
    count = len(refs) - 6 * kinds
    packed, ws, ms, vs, new_w, new_m, new_v = refs[:count], *(refs[at : at + kinds] for at in range(count, len(refs), kinds))
    factor = f_ref[0:1, 0:1]

    def part(which, rows, columns, g):
        at = (0, rows, columns)
        g = g.astype(F32) * factor
        m = 0.9 * ms[which][at] + 0.1 * g
        v = 0.95 * vs[which][at] + 0.05 * g * g
        w = ws[which][at].astype(F32)
        new_w[which][at] = (w - 0.02 * (m * lax.rsqrt(v + 1e-8) + 0.1 * w)).astype(BF)
        new_m[which][at] = m
        new_v[which][at] = v

    def update(number):
        src, at = (head_ref, 0) if number == 0 else (packed[number - 1], packed[number - 1].shape[1] - first)
        every = slice(None)
        for which in range(3):
            width = ws[which].shape[2]
            part(which, every, every, src[:, at : at + width])
            at += width
        src = packed[number]
        d, r = ws[3].shape[2], src.shape[0]
        half, rest = d // 2, ws[3].shape[1] - r
        part(3, slice(0, r), every, src[:, :d])
        part(3, slice(r, r + rest), slice(0, half), src[:rest, d : d + half])
        part(3, slice(r, r + rest), slice(half, d), src[rest:, d : d + half])
        at = d + half
        for which in (4, 5):
            width = ws[which].shape[2]
            part(which, every, every, src[:, at : at + width])
            at += width
        for q in range(0, ws[6].shape[1], r):
            part(6, slice(q, q + r), every, src[:, at : at + d])
            at += d

    for number in range(count):
        pl.when(pl.program_id(0) == number)(functools.partial(update, number))


def adam(factor, head, packed, weights, m, v):
    layers = len(packed)
    one = lambda a: pl.BlockSpec((1, *a.shape[1:]), lambda i: (i, 0, 0))
    arrays = [*weights, *m, *v]
    return pl.pallas_call(
        functools.partial(_adam, first=head.shape[1]),
        grid=(layers,),
        in_specs=[_whole(a.shape) for a in (factor, head, *packed)] + [one(a) for a in arrays],
        out_specs=[one(a) for a in arrays],
        out_shape=[jax.ShapeDtypeStruct(a.shape, a.dtype) for a in arrays],
        compiler_params=_params(),
        cost_estimate=_cost(20 * sum(a.size for a in weights), sum(a.size for a in weights), arrays + arrays),
        name="adam",
    )(factor, head, *packed, *arrays)


def solution(mesh):
    n = mesh.shape["dp"]

    def gathered(x):
        return lax.all_gather(x, "dp", axis=0, tiled=True)

    def scattered(x):
        return lax.psum_scatter(x, "dp", scatter_dimension=0, tiled=True)

    def step(x, dy, *arrays):
        weights, m, v = (arrays[i : i + len(NAMES)] for i in range(0, len(arrays), len(NAMES)))
        layers, ff = weights[0].shape[0], weights[4].shape[2]
        heads = weights[0].shape[2] // HEAD
        first, (head, *packed) = pack(weights)
        fetched = [gathered(packed[0])]
        own, cos, sin = gather(head, tables(x.shape[1]), n, x.shape[1])
        w_attn = [own]
        base = [first] * (layers - 1) + [0]
        h, kept = x[0], []
        for number in range(layers):
            q, k, v_, o, lse = attn_forward(h, w_attn[number], cos, sin, heads)
            kept.append((h, q, k, v_, o, lse))
            if number < layers - 1:
                w_attn.append(fetched[number])
                fetched.append(gathered(lax.optimization_barrier((packed[number + 1], lse))[0]))
                h = mlp_forward(h, o, fetched[number], n, ff, base[number])
        by_h, summed, g_attn = dy[0], [None] * layers, None
        for number in reversed(range(layers)):
            h, q, k, v_, o, lse = kept[number]
            by_mid, by_o, g = mlp_backward(by_h, h, o, fetched[number], n, ff, base[number], g_attn)
            if number < layers - 1:
                g = lax.optimization_barrier((g, summed[number + 1]))[0]
            summed[number] = scattered(g)
            by_h, g_attn = attn_backward(by_mid, by_o, h, q, k, v_, o, lse, w_attn[number], cos, sin, number > 0)
        last = scatter(g_attn, n)
        return tuple(adam(clip([last, *summed], n), last, summed, weights, m, v))

    states, cut = P(("rep", "dp")), P(None, "dp")
    return jax.shard_map(
        step,
        mesh=mesh,
        in_specs=(states, states) + (cut,) * 3 * len(NAMES),
        out_specs=(P("rep", "dp"),) * 3 * len(NAMES),
        check_vma=False,
    )
```
